32 devices in a mesh: corpus: 16 (over z, y, x), dim: 2 (over core).
Axes of the slice: x: 2, y: 2, z: 4, core: 2. Of those that a mesh axis runs over, the one named last changes fastest.
Arguments:
- queries: bfloat16 [128, 768], P('dim'), as said below
- corpus: bfloat16 [8192, 768], P('corpus', 'dim'), as said below
- candidates: int32 [128, 1024], P('dim'), may hold values from 0 to 8191
Outputs:
- log_probs: float32 [128, 1024], P('dim', 'corpus')
The draws below stay inside these ranges and needn't reach their ends.
Inputs may be any that keep to these rules, and one draw needn't show every extreme that they name: `queries`: query rows have real entries of moderate size; their norms differ from row to row. `corpus`: corpus rows have real entries of moderate size; their norms differ from row to row.
All inputs are finite; a program needn't handle non-finite values.
Results may differ from the reference program's by a relative error of at most 0.00095.
Values may be sent and summed in bfloat16 or wider, within the bound.
A program may use at most 64 MiB of HBM per device.

```python
import math
import jax
import jax.numpy as jnp
from jax import lax

D = 768
Q = 128
ROWS_DEV = 512
K = 1024
CORPUS = 8192
N_CORPUS = 16


def corpus_row(key, index):
    base = jax.random.fold_in(key, 11)
    own = jax.random.fold_in(base, index)
    gauss = jax.random.normal(jax.random.fold_in(own, 3), (D,), jnp.float32)
    scale = jnp.exp(jax.random.uniform(jax.random.fold_in(own, 4), (), jnp.float32, math.log(0.5), math.log(1.5)))
    return gauss * scale * 3.0 / math.sqrt(D)


def draw_corpus(key, part):
    indices = jnp.arange(CORPUS, dtype=jnp.int32)
    rows = jax.vmap(lambda index: corpus_row(key, index))(indices)
    return rows.astype(jnp.bfloat16)


def draw_queries(key, part):
    own = jax.random.fold_in(key, 23)
    scales = jnp.exp(jax.random.uniform(jax.random.fold_in(own, 1), (Q, 1), jnp.float32, math.log(0.3), math.log(3.0)))
    drawn = jax.random.normal(jax.random.fold_in(own, 2), (Q, D), jnp.float32) * scales
    return drawn.astype(jnp.bfloat16)


def set_ends(values, stream_key, smallest, largest):
    index_at = [jax.random.randint(jax.random.fold_in(stream_key, axis), (), 0, length) for axis, length in enumerate(values.shape)]
    widest = values.shape.index(max(values.shape))
    neighbour = index_at[:widest] + [(index_at[widest] + 1) % values.shape[widest]] + index_at[widest + 1:]
    return values.at[tuple(index_at)].set(smallest).at[tuple(neighbour)].set(largest)


def setup_inputs(seed: int = 0) -> dict:
    arg_keys = jax.random.split(jax.random.key(seed), 4)
    return {
        "queries": draw_queries(jax.random.fold_in(arg_keys[3], 71), 0),
        "corpus": draw_corpus(jax.random.fold_in(arg_keys[3], 71), 0),
        "candidates": set_ends(jax.random.randint(arg_keys[2], (Q, K), 0, CORPUS), jax.random.fold_in(arg_keys[2], 1), 0, CORPUS - 1).astype(jnp.int32),
    }


def reference(queries, corpus, candidates):
    blocks = corpus.reshape(N_CORPUS, ROWS_DEV, D)

    def absorb(carry, block):
        peak, mass = carry
        scores = lax.dot_general(queries, block, (((1,), (1,)), ((), ())), preferred_element_type=jnp.float32)
        newer = jnp.maximum(peak, jnp.max(scores, axis=1))
        mass = mass * jnp.exp(peak - newer) + jnp.sum(jnp.exp(scores - newer[:, None]), axis=1)
        return (newer, mass), None

    start = (jnp.full((Q,), -1e30, jnp.float32), jnp.zeros((Q,), jnp.float32))
    (peak, mass), unused = lax.scan(absorb, start, blocks)
    lse = peak + jnp.log(mass)

    def score_query(packed):
        query, indices = packed
        chosen = jnp.take(corpus, indices.astype(jnp.int32), axis=0)
        return jnp.dot(chosen, query, preferred_element_type=jnp.float32)

    picked = lax.map(score_query, (queries, candidates))
    return picked - lse[:, None]
```

```python
import functools
import jax
import jax.numpy as jnp
from jax import lax
from jax.experimental import pallas as pl
from jax.experimental.pallas import tpu as pltpu
from jax.sharding import PartitionSpec as P

LANES = 128
MESH = pl.DeviceIdType.MESH


def merged(value, axis, join):
    pieces = jax.tree.map(lambda part: lax.all_gather(part, axis), value)
    head = jax.tree.map(lambda part: part[0], pieces)
    tail = jax.tree.map(lambda part: part[1:], pieces)
    so_far, _ = lax.scan(lambda so_far, section: (join(so_far, section), None), head, tail)
    return so_far


def combine_pair(first, second):
    peak = jnp.maximum(first[0], second[0])
    mass = first[1] * jnp.exp(first[0] - peak) + second[1] * jnp.exp(second[0] - peak)
    return (peak, mass)


def local_pair(scores):
    peak = jnp.max(scores, axis=1)
    mass = jnp.sum(jnp.exp(scores - peak[:, None]), axis=1)
    return (peak, mass)


def pick_owned(scores, indices, offset):
    height = scores.shape[0]
    count = scores.shape[1]
    width = indices.shape[1]
    local = indices - offset
    inside = (local >= 0) & (local < count)
    upper = scores.astype(jnp.bfloat16)
    remain = scores - upper.astype(jnp.float32)
    middle = remain.astype(jnp.bfloat16)
    lower = (remain - middle.astype(jnp.float32)).astype(jnp.bfloat16)
    pieces = jnp.stack([upper, middle, lower], axis=1)
    group = 8

    def select_block(packed):
        block_pieces, block_local = packed
        positions = lax.broadcasted_iota(jnp.int32, (1, 1, count), 2)
        onehot = (block_local[:, :, None] == positions).astype(jnp.bfloat16)
        return jnp.einsum("qkr,qcr->qck", onehot, block_pieces, preferred_element_type=jnp.float32)

    selected = lax.map(
        select_block,
        (
            pieces.reshape(height // group, group, 3, count),
            local.reshape(height // group, group, width),
        ),
    )
    selected = selected.reshape(height, 3, width)
    values = selected[:, 2, :] + selected[:, 1, :] + selected[:, 0, :]
    return jnp.where(inside, values, jnp.float32(0.0))


def plain_body(queries, corpus, candidates):
    rows = corpus.shape[0]
    scores = lax.dot_general(
        queries,
        lax.all_gather(corpus, "dim", axis=1, tiled=True),
        (((1,), (1,)), ((), ())),
        preferred_element_type=jnp.float32,
    )
    peak, mass = merged(local_pair(scores), "corpus", combine_pair)
    own_lse = peak + jnp.log(mass)
    offset = lax.axis_index("corpus") * rows
    picked = pick_owned(scores, candidates, offset)
    logits = lax.psum_scatter(picked, "corpus", scatter_dimension=1, tiled=True)
    return logits - own_lse[:, None]


def times(left, right):
    return lax.dot_general(
        left, right, (((1,), (1,)), ((), ())), preferred_element_type=jnp.float32
    )


def kernel(
    n, q_hbm, c_hbm, k_hbm, out_ref,
    q, own, other, cand, scores, tiles, got, stat, stats,
    load_sem, x_send, x_recv, t_send, t_recv, s_send, s_recv,
):
    me = lax.axis_index("corpus")
    side = lax.axis_index("dim")
    height = q.shape[0]
    rows, feats = own.shape
    width = cand.shape[1] // n
    parts = rows // LANES
    groups = cand.shape[1] // LANES
    half = height // 2

    barrier = pltpu.get_barrier_semaphore()
    pl.semaphore_signal(barrier, inc=1, device_id={"dim": 1 - side}, device_id_type=MESH)
    for step in range(1, n):
        pl.semaphore_signal(
            barrier, inc=1, device_id={"corpus": lax.rem(me + step, n)}, device_id_type=MESH
        )

    def block(b):
        return pl.ds(b * LANES, LANES)

    load_q = pltpu.make_async_copy(q_hbm, q, load_sem.at[0])
    load_k = pltpu.make_async_copy(k_hbm, cand, load_sem.at[1])
    load_c = [
        pltpu.make_async_copy(c_hbm.at[block(b)], own.at[block(b)], load_sem.at[2 + b])
        for b in range(parts)
    ]
    load_q.start()
    for load in load_c:
        load.start()
    load_k.start()
    swaps = [
        pltpu.make_async_remote_copy(
            src_ref=own.at[block(b)],
            dst_ref=other.at[block(b)],
            send_sem=x_send.at[b],
            recv_sem=x_recv.at[b],
            device_id={"dim": 1 - side},
            device_id_type=MESH,
        )
        for b in range(parts)
    ]

    load_q.wait()
    q_own = q[:, pl.ds(pl.multiple_of(side * feats, LANES), feats)]
    for b in range(parts):
        load_c[b].wait()
        scores[:, block(b)] = times(q_own, own[block(b), :])

    pl.semaphore_wait(barrier, n)
    for b in range(parts):
        swaps[b].start()
    load_k.wait()
    q_other = q[:, pl.ds(pl.multiple_of((1 - side) * feats, LANES), feats)]
    for b in range(parts):
        swaps[b].wait_recv()
        scores[:, block(b)] += times(q_other, other[block(b), :])

    def tile_to(p):
        return pltpu.make_async_remote_copy(
            src_ref=tiles.at[p],
            dst_ref=got.at[me],
            send_sem=t_send.at[p],
            recv_sem=t_recv.at[me],
            device_id={"corpus": p},
            device_id_type=MESH,
        )

    first = lax.broadcasted_iota(jnp.int32, (half, LANES), 1) < width
    sends = []
    ready = []
    for step in range(groups):
        away = (step + groups // 2) % groups
        j = lax.rem(me // 2 + away, groups)
        local = cand[:, pl.ds(pl.multiple_of(j * LANES, LANES), LANES)] - me * rows
        lane = local & (LANES - 1)
        part = lax.shift_right_arithmetic(local, LANES.bit_length() - 1)
        picked = jnp.zeros((height, LANES), jnp.float32)
        for b in range(parts):
            found = jnp.take_along_axis(
                scores[:, block(b)], lane, axis=1, mode="promise_in_bounds"
            )
            picked = jnp.where(part == b, found, picked)
        low, high = picked[:half], picked[half:]
        tiles[2 * j] = jnp.where(first, low, pltpu.roll(high, width, 1)).astype(tiles.dtype)
        tiles[2 * j + 1] = jnp.where(first, pltpu.roll(low, width, 1), high).astype(tiles.dtype)
        for copy in ready:
            copy.start()
        sends += ready
        if away:
            ready = [tile_to(2 * j), tile_to(2 * j + 1)]
        else:
            ready = [tile_to(2 * j + 1 - lax.rem(me, 2))]

    peak = jnp.max(scores[...], axis=1, keepdims=True)
    mass = jnp.sum(jnp.exp(scores[...] - peak), axis=1, keepdims=True)
    lse = peak + jnp.log(mass)
    for copy in ready:
        copy.start()
    sends += ready
    square = lax.broadcasted_iota(jnp.int32, (height, LANES), 0) == lax.broadcasted_iota(
        jnp.int32, (height, LANES), 1
    )
    stat[...] = jnp.sum(jnp.where(square, lse, 0.0), axis=0, keepdims=True)
    for step in range(1, n):
        p = lax.rem(me + step, n)
        copy = pltpu.make_async_remote_copy(
            src_ref=stat,
            dst_ref=stats.at[me],
            send_sem=s_send.at[p],
            recv_sem=s_recv.at[me],
            device_id={"corpus": p},
            device_id_type=MESH,
        )
        copy.start()
        sends.append(copy)

    total = tiles[me].astype(jnp.float32)
    lines = [stat[...]]
    for step in range(1, n):
        p = lax.rem(me + step, n)
        pltpu.make_async_remote_copy(
            src_ref=tiles.at[p],
            dst_ref=got.at[p],
            send_sem=t_send.at[p],
            recv_sem=t_recv.at[p],
            device_id={"corpus": p},
            device_id_type=MESH,
        ).wait_recv()
        total += got[p].astype(jnp.float32)
    for step in range(1, n):
        p = lax.rem(me + step, n)
        pltpu.make_async_remote_copy(
            src_ref=stat,
            dst_ref=stats.at[p],
            send_sem=s_send.at[p],
            recv_sem=s_recv.at[p],
            device_id={"corpus": p},
            device_id_type=MESH,
        ).wait_recv()
        lines.append(stats[p])
    top = functools.reduce(jnp.maximum, lines)
    line = top + jnp.log(sum(jnp.exp(item - top) for item in lines))
    column = jnp.sum(jnp.where(square, line, 0.0), axis=1, keepdims=True)
    result = total - jnp.where(first, column[:half], column[half:])
    out_ref[pl.ds(0, half), :] = result[:, :width]
    out_ref[pl.ds(half, half), :] = pltpu.roll(result, width, 1)[:, :width]

    for copy in swaps + sends:
        copy.wait_send()


def fused_body(n, queries, corpus, candidates):
    height, depth = queries.shape
    rows, feats = corpus.shape
    count = candidates.shape[1]
    parts = rows // LANES
    width = count // n
    dma = pltpu.SemaphoreType.DMA
    return pl.pallas_call(
        functools.partial(kernel, n),
        out_shape=jax.ShapeDtypeStruct((height, width), jnp.float32),
        in_specs=[pl.BlockSpec(memory_space=pl.ANY)] * 3,
        out_specs=pl.BlockSpec(memory_space=pltpu.VMEM),
        scratch_shapes=[
            pltpu.VMEM((height, depth), queries.dtype),
            pltpu.VMEM((rows, feats), corpus.dtype),
            pltpu.VMEM((rows, feats), corpus.dtype),
            pltpu.VMEM((height, count), jnp.int32),
            pltpu.VMEM((height, rows), jnp.float32),
            pltpu.VMEM((n, height // 2, LANES), jnp.bfloat16),
            pltpu.VMEM((n, height // 2, LANES), jnp.bfloat16),
            pltpu.VMEM((1, LANES), jnp.float32),
            pltpu.VMEM((n, 1, LANES), jnp.float32),
            dma((2 + parts,)),
            dma((parts,)),
            dma((parts,)),
            dma((n,)),
            dma((n,)),
            dma((n,)),
            dma((n,)),
        ],
        compiler_params=pltpu.CompilerParams(collective_id=0, has_side_effects=True),
    )(queries, corpus, candidates)


def body(n, cores, queries, corpus, candidates):
    dense = (
        cores == 2
        and candidates.shape[1] == n * LANES // 2
        and n % 2 == 0
        and queries.shape[0] <= LANES
        and queries.shape[0] % 32 == 0
        and corpus.shape[0] % LANES == 0
        and corpus.shape[1] % LANES == 0
    )
    if dense:
        return fused_body(n, queries, corpus, candidates)
    return plain_body(queries, corpus, candidates)


def solution(mesh):
    placed = (P("dim", None), P("corpus", "dim"), P("dim", None))
    sized = functools.partial(body, mesh.shape["corpus"], mesh.shape["dim"])
    return jax.shard_map(
        sized, mesh=mesh, in_specs=placed, out_specs=P("dim", "corpus"), check_vma=False
    )
```

```python
import functools
import jax
import jax.numpy as jnp
from jax import lax
from jax.experimental import pallas as pl
from jax.experimental.pallas import tpu as pltpu
from jax.sharding import PartitionSpec as P

LANES = 128
MESH = pl.DeviceIdType.MESH


def merged(value, axis, join):
    pieces = jax.tree.map(lambda part: lax.all_gather(part, axis), value)
    head = jax.tree.map(lambda part: part[0], pieces)
    tail = jax.tree.map(lambda part: part[1:], pieces)
    so_far, _ = lax.scan(lambda so_far, section: (join(so_far, section), None), head, tail)
    return so_far


def combine_pair(first, second):
    peak = jnp.maximum(first[0], second[0])
    mass = first[1] * jnp.exp(first[0] - peak) + second[1] * jnp.exp(second[0] - peak)
    return (peak, mass)


def local_pair(scores):
    peak = jnp.max(scores, axis=1)
    mass = jnp.sum(jnp.exp(scores - peak[:, None]), axis=1)
    return (peak, mass)


def pick_owned(scores, indices, offset):
    height = scores.shape[0]
    count = scores.shape[1]
    width = indices.shape[1]
    local = indices - offset
    inside = (local >= 0) & (local < count)
    upper = scores.astype(jnp.bfloat16)
    remain = scores - upper.astype(jnp.float32)
    middle = remain.astype(jnp.bfloat16)
    lower = (remain - middle.astype(jnp.float32)).astype(jnp.bfloat16)
    pieces = jnp.stack([upper, middle, lower], axis=1)
    group = 8

    def select_block(packed):
        block_pieces, block_local = packed
        positions = lax.broadcasted_iota(jnp.int32, (1, 1, count), 2)
        onehot = (block_local[:, :, None] == positions).astype(jnp.bfloat16)
        return jnp.einsum("qkr,qcr->qck", onehot, block_pieces, preferred_element_type=jnp.float32)

    selected = lax.map(
        select_block,
        (
            pieces.reshape(height // group, group, 3, count),
            local.reshape(height // group, group, width),
        ),
    )
    selected = selected.reshape(height, 3, width)
    values = selected[:, 2, :] + selected[:, 1, :] + selected[:, 0, :]
    return jnp.where(inside, values, jnp.float32(0.0))


def plain_body(queries, corpus, candidates):
    rows = corpus.shape[0]
    scores = lax.dot_general(
        queries,
        lax.all_gather(corpus, "dim", axis=1, tiled=True),
        (((1,), (1,)), ((), ())),
        preferred_element_type=jnp.float32,
    )
    peak, mass = merged(local_pair(scores), "corpus", combine_pair)
    own_lse = peak + jnp.log(mass)
    offset = lax.axis_index("corpus") * rows
    picked = pick_owned(scores, candidates, offset)
    logits = lax.psum_scatter(picked, "corpus", scatter_dimension=1, tiled=True)
    return logits - own_lse[:, None]


def times(left, right):
    return lax.dot_general(
        left, right, (((1,), (1,)), ((), ())), preferred_element_type=jnp.float32
    )


def kernel(
    n, q_hbm, c_hbm, k_hbm, out_ref,
    q, own, other, cand, scores, tiles, got, stat, stats,
    wave, load_sem, x_send, x_recv, t_send, t_recv, s_send, s_recv,
):
    me = lax.axis_index("corpus")
    side = lax.axis_index("dim")
    height = q.shape[0]
    rows, feats = own.shape
    width = cand.shape[1] // n
    parts = rows // LANES
    groups = cand.shape[1] // LANES
    half = height // 2

    def across(bit):
        return me + bit - 2 * bit * lax.rem(me // bit, 2)

    barrier = pltpu.get_barrier_semaphore()
    bits = [1 << i for i in range(n.bit_length() - 1)]
    pl.semaphore_signal(barrier, inc=1, device_id={"dim": 1 - side}, device_id_type=MESH)
    for bit in bits:
        pl.semaphore_signal(
            barrier, inc=1, device_id={"corpus": across(bit)}, device_id_type=MESH
        )

    def block(b):
        return pl.ds(b * LANES, LANES)

    load_q = pltpu.make_async_copy(q_hbm, q, load_sem.at[0])
    load_k = pltpu.make_async_copy(k_hbm, cand, load_sem.at[1])
    load_c = [
        pltpu.make_async_copy(c_hbm.at[block(b)], own.at[block(b)], load_sem.at[2 + b])
        for b in range(parts)
    ]
    for load in load_c:
        load.start()
    load_q.start()
    load_k.start()
    swaps = [
        pltpu.make_async_remote_copy(
            src_ref=own.at[block(b)],
            dst_ref=other.at[block(b)],
            send_sem=x_send.at[b],
            recv_sem=x_recv.at[b],
            device_id={"dim": 1 - side},
            device_id_type=MESH,
        )
        for b in range(parts)
    ]

    def tell(i):
        pl.semaphore_signal(
            wave.at[i], inc=1, device_id={"corpus": across(bits[i])}, device_id_type=MESH
        )

    pl.semaphore_wait(barrier, len(bits) + 1)
    rounds = len(bits) - 1
    tell(0)
    for b in range(parts):
        load_c[b].wait()
        swaps[b].start()
    load_q.wait()
    q_own = q[:, pl.ds(pl.multiple_of(side * feats, LANES), feats)]
    q_other = q[:, pl.ds(pl.multiple_of((1 - side) * feats, LANES), feats)]
    for b in range(parts):
        scores[:, block(b)] = times(q_own, own[block(b), :])
    pl.semaphore_wait(wave.at[0], 1)
    tell(1)
    load_k.wait()
    for b in range(parts):
        swaps[b].wait_recv()
        scores[:, block(b)] += times(q_other, other[block(b), :])
        if b == parts // 2 - 1:
            pl.semaphore_wait(wave.at[1], 1)
            tell(2)
    for i in range(2, rounds):
        pl.semaphore_wait(wave.at[i], 1)
        if i + 1 < rounds:
            tell(i + 1)

    def tile_to(p):
        return pltpu.make_async_remote_copy(
            src_ref=tiles.at[p],
            dst_ref=got.at[me],
            send_sem=t_send.at[p],
            recv_sem=t_recv.at[me],
            device_id={"corpus": p},
            device_id_type=MESH,
        )

    first = lax.broadcasted_iota(jnp.int32, (half, LANES), 1) < width
    square = lax.broadcasted_iota(jnp.int32, (height, LANES), 0) == lax.broadcasted_iota(
        jnp.int32, (height, LANES), 1
    )
    sends = []
    ready = []

    def send_stats():
        peak = jnp.max(scores[...], axis=1, keepdims=True)
        mass = jnp.sum(jnp.exp(scores[...] - peak), axis=1, keepdims=True)
        lse = peak + jnp.log(mass)
        stat[...] = jnp.sum(jnp.where(square, lse, 0.0), axis=0, keepdims=True)
        for step in range(1, n):
            p = lax.rem(me + step, n)
            copy = pltpu.make_async_remote_copy(
                src_ref=stat,
                dst_ref=stats.at[me],
                send_sem=s_send.at[p],
                recv_sem=s_recv.at[me],
                device_id={"corpus": p},
                device_id_type=MESH,
            )
            copy.start()
            sends.append(copy)

    for step in range(groups):
        away = (step + groups // 2) % groups
        j = lax.rem(me // 2 + away, groups)
        local = cand[:, pl.ds(pl.multiple_of(j * LANES, LANES), LANES)] - me * rows
        lane = local & (LANES - 1)
        part = lax.shift_right_arithmetic(local, LANES.bit_length() - 1)
        picked = jnp.zeros((height, LANES), jnp.float32)
        for b in range(parts):
            found = jnp.take_along_axis(
                scores[:, block(b)], lane, axis=1, mode="promise_in_bounds"
            )
            picked = jnp.where(part == b, found, picked)
        low, high = picked[:half], picked[half:]
        tiles[2 * j] = jnp.where(first, low, pltpu.roll(high, width, 1)).astype(tiles.dtype)
        tiles[2 * j + 1] = jnp.where(first, pltpu.roll(low, width, 1), high).astype(tiles.dtype)
        for copy in ready:
            copy.start()
        sends += ready
        if step == groups // 2:
            send_stats()
        if away:
            ready = [tile_to(2 * j), tile_to(2 * j + 1)]
        else:
            ready = [tile_to(2 * j + 1 - lax.rem(me, 2))]

    for copy in ready:
        copy.start()
    sends += ready

    total = tiles[me].astype(jnp.float32)
    lines = [stat[...]]
    for step in range(1, n):
        p = lax.rem(me + step, n)
        pltpu.make_async_remote_copy(
            src_ref=tiles.at[p],
            dst_ref=got.at[p],
            send_sem=t_send.at[p],
            recv_sem=t_recv.at[p],
            device_id={"corpus": p},
            device_id_type=MESH,
        ).wait_recv()
        total += got[p].astype(jnp.float32)
    for step in range(1, n):
        p = lax.rem(me + step, n)
        pltpu.make_async_remote_copy(
            src_ref=stat,
            dst_ref=stats.at[p],
            send_sem=s_send.at[p],
            recv_sem=s_recv.at[p],
            device_id={"corpus": p},
            device_id_type=MESH,
        ).wait_recv()
        lines.append(stats[p])
    top = functools.reduce(jnp.maximum, lines)
    line = top + jnp.log(sum(jnp.exp(item - top) for item in lines))
    column = jnp.sum(jnp.where(square, line, 0.0), axis=1, keepdims=True)
    result = total - jnp.where(first, column[:half], column[half:])
    out_ref[pl.ds(0, half), :] = result[:, :width]
    out_ref[pl.ds(half, half), :] = pltpu.roll(result, width, 1)[:, :width]

    for copy in swaps + sends:
        copy.wait_send()


def fused_body(n, queries, corpus, candidates):
    height, depth = queries.shape
    rows, feats = corpus.shape
    count = candidates.shape[1]
    parts = rows // LANES
    width = count // n
    dma = pltpu.SemaphoreType.DMA
    return pl.pallas_call(
        functools.partial(kernel, n),
        out_shape=jax.ShapeDtypeStruct((height, width), jnp.float32),
        in_specs=[pl.BlockSpec(memory_space=pltpu.HBM)] * 3,
        out_specs=pl.BlockSpec(memory_space=pltpu.VMEM),
        scratch_shapes=[
            pltpu.VMEM((height, depth), queries.dtype),
            pltpu.VMEM((rows, feats), corpus.dtype),
            pltpu.VMEM((rows, feats), corpus.dtype),
            pltpu.VMEM((height, count), jnp.int32),
            pltpu.VMEM((height, rows), jnp.float32),
            pltpu.VMEM((n, height // 2, LANES), jnp.bfloat16),
            pltpu.VMEM((n, height // 2, LANES), jnp.bfloat16),
            pltpu.VMEM((1, LANES), jnp.float32),
            pltpu.VMEM((n, 1, LANES), jnp.float32),
            pltpu.SemaphoreType.REGULAR((n.bit_length() - 2,)),
            dma((2 + parts,)),
            dma((parts,)),
            dma((parts,)),
            dma((n,)),
            dma((n,)),
            dma((n,)),
            dma((n,)),
        ],
        compiler_params=pltpu.CompilerParams(collective_id=0, has_side_effects=True),
    )(queries, corpus, candidates)


def body(n, cores, queries, corpus, candidates):
    dense = (
        cores == 2
        and candidates.shape[1] == n * LANES // 2
        and n >= 16
        and n & (n - 1) == 0
        and queries.shape[0] <= LANES
        and queries.shape[0] % 32 == 0
        and corpus.shape[0] % LANES == 0
        and corpus.shape[1] % LANES == 0
    )
    if dense:
        return fused_body(n, queries, corpus, candidates)
    return plain_body(queries, corpus, candidates)


def solution(mesh):
    placed = (P("dim", None), P("corpus", "dim"), P("dim", None))
    sized = functools.partial(body, mesh.shape["corpus"], mesh.shape["dim"])
    return jax.shard_map(
        sized, mesh=mesh, in_specs=placed, out_specs=P("dim", "corpus"), check_vma=False
    )
```

```python
import functools
import jax
import jax.numpy as jnp
from jax import lax
from jax.experimental import pallas as pl
from jax.experimental.pallas import tpu as pltpu
from jax.sharding import PartitionSpec as P

LANES = 128
ROOM = 55169 << 10
MESH = pl.DeviceIdType.MESH


def merged(value, axis, join):
    pieces = jax.tree.map(lambda part: lax.all_gather(part, axis), value)
    head = jax.tree.map(lambda part: part[0], pieces)
    tail = jax.tree.map(lambda part: part[1:], pieces)
    so_far, _ = lax.scan(lambda so_far, section: (join(so_far, section), None), head, tail)
    return so_far


def combine_pair(first, second):
    peak = jnp.maximum(first[0], second[0])
    mass = first[1] * jnp.exp(first[0] - peak) + second[1] * jnp.exp(second[0] - peak)
    return (peak, mass)


def local_pair(scores):
    peak = jnp.max(scores, axis=1)
    mass = jnp.sum(jnp.exp(scores - peak[:, None]), axis=1)
    return (peak, mass)


def pick_owned(scores, indices, offset):
    height = scores.shape[0]
    count = scores.shape[1]
    width = indices.shape[1]
    local = indices - offset
    inside = (local >= 0) & (local < count)
    upper = scores.astype(jnp.bfloat16)
    remain = scores - upper.astype(jnp.float32)
    middle = remain.astype(jnp.bfloat16)
    lower = (remain - middle.astype(jnp.float32)).astype(jnp.bfloat16)
    pieces = jnp.stack([upper, middle, lower], axis=1)
    group = 8

    def select_block(packed):
        block_pieces, block_local = packed
        positions = lax.broadcasted_iota(jnp.int32, (1, 1, count), 2)
        onehot = (block_local[:, :, None] == positions).astype(jnp.bfloat16)
        return jnp.einsum("qkr,qcr->qck", onehot, block_pieces, preferred_element_type=jnp.float32)

    selected = lax.map(
        select_block,
        (
            pieces.reshape(height // group, group, 3, count),
            local.reshape(height // group, group, width),
        ),
    )
    selected = selected.reshape(height, 3, width)
    values = selected[:, 2, :] + selected[:, 1, :] + selected[:, 0, :]
    return jnp.where(inside, values, jnp.float32(0.0))


def plain_body(queries, corpus, candidates):
    rows = corpus.shape[0]
    scores = lax.dot_general(
        queries,
        lax.all_gather(corpus, "dim", axis=1, tiled=True),
        (((1,), (1,)), ((), ())),
        preferred_element_type=jnp.float32,
    )
    peak, mass = merged(local_pair(scores), "corpus", combine_pair)
    own_lse = peak + jnp.log(mass)
    offset = lax.axis_index("corpus") * rows
    picked = pick_owned(scores, candidates, offset)
    logits = lax.psum_scatter(picked, "corpus", scatter_dimension=1, tiled=True)
    return logits - own_lse[:, None]


def times(left, right):
    return lax.dot_general(
        left, right, (((1,), (1,)), ((), ())), preferred_element_type=jnp.float32
    )


def kernel(
    n, q_hbm, c_hbm, k_hbm, out_ref,
    q, own, other, cand, scores, tiles, got, stat, stats,
    wave, load_sem, x_send, x_recv, t_send, t_recv, s_send, s_recv,
):
    me = lax.axis_index("corpus")
    side = lax.axis_index("dim")
    height = q.shape[0]
    rows, feats = own.shape
    width = cand.shape[1] // n
    parts = rows // LANES
    groups = cand.shape[1] // LANES
    half = height // 2

    def across(bit):
        return me + bit - 2 * bit * lax.rem(me // bit, 2)

    barrier = pltpu.get_barrier_semaphore()
    bits = [1 << i for i in range(n.bit_length() - 1)]
    pl.semaphore_signal(barrier, inc=1, device_id={"dim": 1 - side}, device_id_type=MESH)
    for bit in bits:
        pl.semaphore_signal(
            barrier, inc=1, device_id={"corpus": across(bit)}, device_id_type=MESH
        )

    def block(b):
        return pl.ds(b * LANES, LANES)

    load_q = pltpu.make_async_copy(q_hbm, q, load_sem.at[0])
    load_k = pltpu.make_async_copy(k_hbm, cand, load_sem.at[1])
    load_c = [
        pltpu.make_async_copy(c_hbm.at[block(b)], own.at[block(b)], load_sem.at[2 + b])
        for b in range(parts)
    ]
    for load in load_c:
        load.start()
    load_q.start()
    load_k.start()
    swaps = [
        pltpu.make_async_remote_copy(
            src_ref=own.at[block(b)],
            dst_ref=other.at[block(b)],
            send_sem=x_send.at[b],
            recv_sem=x_recv.at[b],
            device_id={"dim": 1 - side},
            device_id_type=MESH,
        )
        for b in range(parts)
    ]

    def tell(i):
        pl.semaphore_signal(
            wave.at[i], inc=1, device_id={"corpus": across(bits[i])}, device_id_type=MESH
        )

    pl.semaphore_wait(barrier, len(bits) + 1)
    tell(0)
    for b in range(parts):
        load_c[b].wait()
        swaps[b].start()
    load_q.wait()
    q_own = q[:, pl.ds(pl.multiple_of(side * feats, LANES), feats)]
    q_other = q[:, pl.ds(pl.multiple_of((1 - side) * feats, LANES), feats)]
    for b in range(parts):
        scores[:, block(b)] = times(q_own, own[block(b), :])
    for i in range(1, len(bits) - 1):
        pl.semaphore_wait(wave.at[i - 1], 1)
        tell(i)
    load_k.wait()
    for b in range(parts):
        swaps[b].wait_recv()
        scores[:, block(b)] += times(q_other, other[block(b), :])

    def tile_to(p):
        return pltpu.make_async_remote_copy(
            src_ref=tiles.at[p],
            dst_ref=got.at[me],
            send_sem=t_send.at[p],
            recv_sem=t_recv.at[me],
            device_id={"corpus": p},
            device_id_type=MESH,
        )

    first = lax.broadcasted_iota(jnp.int32, (half, LANES), 1) < width
    square = lax.broadcasted_iota(jnp.int32, (height, LANES), 0) == lax.broadcasted_iota(
        jnp.int32, (height, LANES), 1
    )
    sends = []
    ready = []

    def send_stats():
        peak = jnp.max(scores[...], axis=1, keepdims=True)
        mass = jnp.sum(jnp.exp(scores[...] - peak), axis=1, keepdims=True)
        lse = peak + jnp.log(mass)
        stat[...] = jnp.sum(jnp.where(square, lse, 0.0), axis=0, keepdims=True)
        for step in range(1, n):
            p = lax.rem(me + step, n)
            copy = pltpu.make_async_remote_copy(
                src_ref=stat,
                dst_ref=stats.at[me],
                send_sem=s_send.at[p],
                recv_sem=s_recv.at[me],
                device_id={"corpus": p},
                device_id_type=MESH,
            )
            copy.start()
            sends.append(copy)

    for step in range(groups):
        away = (step + groups // 2) % groups
        j = lax.rem(me // 2 + away, groups)
        local = cand[:, pl.ds(pl.multiple_of(j * LANES, LANES), LANES)] - me * rows
        lane = local & (LANES - 1)
        part = lax.shift_right_arithmetic(local, LANES.bit_length() - 1)
        picked = jnp.zeros((height, LANES), jnp.float32)
        for b in range(parts):
            found = jnp.take_along_axis(
                scores[:, block(b)], lane, axis=1, mode="promise_in_bounds"
            )
            picked = jnp.where(part == b, found, picked)
        low, high = picked[:half], picked[half:]
        tiles[2 * j] = jnp.where(first, low, pltpu.roll(high, width, 1)).astype(tiles.dtype)
        tiles[2 * j + 1] = jnp.where(first, pltpu.roll(low, width, 1), high).astype(tiles.dtype)
        if step == 0:
            pl.semaphore_wait(wave.at[len(bits) - 2], 1)
        for copy in ready:
            copy.start()
        sends += ready
        if step == groups // 2:
            send_stats()
        if away:
            ready = [tile_to(2 * j), tile_to(2 * j + 1)]
        else:
            ready = [tile_to(2 * j + 1 - lax.rem(me, 2))]

    for copy in ready:
        copy.start()
    sends += ready

    total = tiles[me].astype(jnp.float32)
    lines = [stat[...]]
    for step in range(1, n):
        p = lax.rem(me + step, n)
        pltpu.make_async_remote_copy(
            src_ref=tiles.at[p],
            dst_ref=got.at[p],
            send_sem=t_send.at[p],
            recv_sem=t_recv.at[p],
            device_id={"corpus": p},
            device_id_type=MESH,
        ).wait_recv()
        total += got[p].astype(jnp.float32)
    for step in range(1, n):
        p = lax.rem(me + step, n)
        pltpu.make_async_remote_copy(
            src_ref=stat,
            dst_ref=stats.at[p],
            send_sem=s_send.at[p],
            recv_sem=s_recv.at[p],
            device_id={"corpus": p},
            device_id_type=MESH,
        ).wait_recv()
        lines.append(stats[p])
    top = functools.reduce(jnp.maximum, lines)
    line = top + jnp.log(sum(jnp.exp(item - top) for item in lines))
    column = jnp.sum(jnp.where(square, line, 0.0), axis=1, keepdims=True)
    result = total - jnp.where(first, column[:half], column[half:])
    out_ref[pl.ds(0, half), :] = result[:, :width]
    out_ref[pl.ds(half, half), :] = pltpu.roll(result, width, 1)[:, :width]

    for copy in swaps + sends:
        copy.wait_send()


def fused_body(n, queries, corpus, candidates):
    height, depth = queries.shape
    rows, feats = corpus.shape
    count = candidates.shape[1]
    parts = rows // LANES
    width = count // n
    dma = pltpu.SemaphoreType.DMA
    return pl.pallas_call(
        functools.partial(kernel, n),
        out_shape=jax.ShapeDtypeStruct((height, width), jnp.float32),
        in_specs=[pl.BlockSpec(memory_space=pltpu.HBM)] * 3,
        out_specs=pl.BlockSpec(memory_space=pltpu.VMEM),
        scratch_shapes=[
            pltpu.VMEM((height, depth), queries.dtype),
            pltpu.VMEM((rows, feats), corpus.dtype),
            pltpu.VMEM((rows, feats), corpus.dtype),
            pltpu.VMEM((height, count), jnp.int32),
            pltpu.VMEM((height, rows), jnp.float32),
            pltpu.VMEM((n, height // 2, LANES), jnp.bfloat16),
            pltpu.VMEM((n, height // 2, LANES), jnp.bfloat16),
            pltpu.VMEM((1, LANES), jnp.float32),
            pltpu.VMEM((n, 1, LANES), jnp.float32),
            pltpu.SemaphoreType.REGULAR((n.bit_length() - 2,)),
            dma((2 + parts,)),
            dma((parts,)),
            dma((parts,)),
            dma((n,)),
            dma((n,)),
            dma((n,)),
            dma((n,)),
        ],
        compiler_params=pltpu.CompilerParams(
            collective_id=0, has_side_effects=True, vmem_limit_bytes=ROOM
        ),
    )(queries, corpus, candidates)


def body(n, cores, queries, corpus, candidates):
    dense = (
        cores == 2
        and candidates.shape[1] == n * LANES // 2
        and n >= 16
        and n & (n - 1) == 0
        and queries.shape[0] <= LANES
        and queries.shape[0] % 32 == 0
        and corpus.shape[0] % LANES == 0
        and corpus.shape[1] % LANES == 0
    )
    if dense:
        return fused_body(n, queries, corpus, candidates)
    return plain_body(queries, corpus, candidates)


def solution(mesh):
    placed = (P("dim", None), P("corpus", "dim"), P("dim", None))
    sized = functools.partial(body, mesh.shape["corpus"], mesh.shape["dim"])
    return jax.shard_map(
        sized, mesh=mesh, in_specs=placed, out_specs=P("dim", "corpus"), check_vma=False
    )
```

```python
import functools
import jax
import jax.numpy as jnp
from jax import lax
from jax.experimental import pallas as pl
from jax.experimental.pallas import tpu as pltpu
from jax.sharding import PartitionSpec as P

LANES = 128
ROOM = 55169 << 10
MESH = pl.DeviceIdType.MESH


def merged(value, axis, join):
    pieces = jax.tree.map(lambda part: lax.all_gather(part, axis), value)
    head = jax.tree.map(lambda part: part[0], pieces)
    tail = jax.tree.map(lambda part: part[1:], pieces)
    so_far, _ = lax.scan(lambda so_far, section: (join(so_far, section), None), head, tail)
    return so_far


def combine_pair(first, second):
    peak = jnp.maximum(first[0], second[0])
    mass = first[1] * jnp.exp(first[0] - peak) + second[1] * jnp.exp(second[0] - peak)
    return (peak, mass)


def local_pair(scores):
    peak = jnp.max(scores, axis=1)
    mass = jnp.sum(jnp.exp(scores - peak[:, None]), axis=1)
    return (peak, mass)


def pick_owned(scores, indices, offset):
    height = scores.shape[0]
    count = scores.shape[1]
    width = indices.shape[1]
    local = indices - offset
    inside = (local >= 0) & (local < count)
    upper = scores.astype(jnp.bfloat16)
    remain = scores - upper.astype(jnp.float32)
    middle = remain.astype(jnp.bfloat16)
    lower = (remain - middle.astype(jnp.float32)).astype(jnp.bfloat16)
    pieces = jnp.stack([upper, middle, lower], axis=1)
    group = 8

    def select_block(packed):
        block_pieces, block_local = packed
        positions = lax.broadcasted_iota(jnp.int32, (1, 1, count), 2)
        onehot = (block_local[:, :, None] == positions).astype(jnp.bfloat16)
        return jnp.einsum("qkr,qcr->qck", onehot, block_pieces, preferred_element_type=jnp.float32)

    selected = lax.map(
        select_block,
        (
            pieces.reshape(height // group, group, 3, count),
            local.reshape(height // group, group, width),
        ),
    )
    selected = selected.reshape(height, 3, width)
    values = selected[:, 2, :] + selected[:, 1, :] + selected[:, 0, :]
    return jnp.where(inside, values, jnp.float32(0.0))


def plain_body(queries, corpus, candidates):
    rows = corpus.shape[0]
    scores = lax.dot_general(
        queries,
        lax.all_gather(corpus, "dim", axis=1, tiled=True),
        (((1,), (1,)), ((), ())),
        preferred_element_type=jnp.float32,
    )
    peak, mass = merged(local_pair(scores), "corpus", combine_pair)
    own_lse = peak + jnp.log(mass)
    offset = lax.axis_index("corpus") * rows
    picked = pick_owned(scores, candidates, offset)
    logits = lax.psum_scatter(picked, "corpus", scatter_dimension=1, tiled=True)
    return logits - own_lse[:, None]


def times(left, right):
    return lax.dot_general(
        left, right, (((1,), (1,)), ((), ())), preferred_element_type=jnp.float32
    )


def kernel(
    n, q_hbm, c_hbm, k_hbm, out_ref,
    q, own, other, cand, scores, tiles, got, stat, stats,
    wave, load_sem, x_send, x_recv, t_send, t_recv, s_send, s_recv,
):
    me = lax.axis_index("corpus")
    side = lax.axis_index("dim")
    height = q.shape[0]
    rows, feats = own.shape
    width = cand.shape[1] // n
    parts = rows // LANES
    groups = cand.shape[1] // LANES
    half = height // 2

    def flipped(value, mask):
        for i in range(mask.bit_length()):
            bit = 1 << i
            if mask & bit:
                value = value + bit - 2 * bit * lax.rem(value // bit, 2)
        return value

    barrier = pltpu.get_barrier_semaphore()
    partner_in, all_in = wave.at[0], wave.at[1]

    def tell_partner(semaphore):
        pl.semaphore_signal(
            semaphore, inc=1, device_id={"dim": 1 - side}, device_id_type=MESH
        )

    @pl.when(side == 0)
    def _():
        tell_partner(barrier)

    def block(b):
        return pl.ds(b * LANES, LANES)

    load_q = pltpu.make_async_copy(q_hbm, q, load_sem.at[0])
    load_k = pltpu.make_async_copy(k_hbm, cand, load_sem.at[1])
    load_c = [
        pltpu.make_async_copy(c_hbm.at[block(b)], own.at[block(b)], load_sem.at[2 + b])
        for b in range(parts)
    ]
    for load in load_c:
        load.start()
    load_q.start()
    load_k.start()
    swaps = [
        pltpu.make_async_remote_copy(
            src_ref=own.at[block(b)],
            dst_ref=other.at[block(b)],
            send_sem=x_send.at[b],
            recv_sem=x_recv.at[b],
            device_id={"dim": 1 - side},
            device_id_type=MESH,
        )
        for b in range(parts)
    ]

    @pl.when(side == 1)
    def _():
        pl.semaphore_wait(barrier, 1)
        tell_partner(partner_in)

    @pl.when(side == 0)
    def _():
        pl.semaphore_wait(partner_in, 1)
        for step in range(1, n):
            pl.semaphore_signal(
                barrier, inc=1, device_id={"corpus": lax.rem(me + step, n)}, device_id_type=MESH
            )

    for b in range(parts):
        load_c[b].wait()
        swaps[b].start()
    load_q.wait()
    q_own = q[:, pl.ds(pl.multiple_of(side * feats, LANES), feats)]
    q_other = q[:, pl.ds(pl.multiple_of((1 - side) * feats, LANES), feats)]
    for b in range(parts):
        scores[:, block(b)] = times(q_own, own[block(b), :])
    load_k.wait()
    for b in range(parts):
        swaps[b].wait_recv()
        scores[:, block(b)] += times(q_other, other[block(b), :])

    def wait_for_all():
        @pl.when(side == 0)
        def _():
            pl.semaphore_wait(barrier, n - 1)
            tell_partner(all_in)

        @pl.when(side == 1)
        def _():
            pl.semaphore_wait(all_in, 1)

    def tile_to(p):
        return pltpu.make_async_remote_copy(
            src_ref=tiles.at[p],
            dst_ref=got.at[me],
            send_sem=t_send.at[p],
            recv_sem=t_recv.at[me],
            device_id={"corpus": p},
            device_id_type=MESH,
        )

    first = lax.broadcasted_iota(jnp.int32, (half, LANES), 1) < width
    square = lax.broadcasted_iota(jnp.int32, (height, LANES), 0) == lax.broadcasted_iota(
        jnp.int32, (height, LANES), 1
    )
    sends = []
    ready = []

    def send_stats():
        peak = jnp.max(scores[...], axis=1, keepdims=True)
        mass = jnp.sum(jnp.exp(scores[...] - peak), axis=1, keepdims=True)
        lse = peak + jnp.log(mass)
        stat[...] = jnp.sum(jnp.where(square, lse, 0.0), axis=0, keepdims=True)
        for step in range(1, n):
            p = lax.rem(me + step, n)
            copy = pltpu.make_async_remote_copy(
                src_ref=stat,
                dst_ref=stats.at[me],
                send_sem=s_send.at[p],
                recv_sem=s_recv.at[me],
                device_id={"corpus": p},
                device_id_type=MESH,
            )
            copy.start()
            sends.append(copy)

    for step in range(groups):
        away = groups - 1 - step
        j = flipped(me // 2, away)
        local = cand[:, pl.ds(pl.multiple_of(j * LANES, LANES), LANES)] - me * rows
        lane = local & (LANES - 1)
        part = lax.shift_right_arithmetic(local, LANES.bit_length() - 1)
        picked = jnp.zeros((height, LANES), jnp.float32)
        for b in range(parts):
            found = jnp.take_along_axis(
                scores[:, block(b)], lane, axis=1, mode="promise_in_bounds"
            )
            picked = jnp.where(part == b, found, picked)
        low, high = picked[:half], picked[half:]
        tiles[2 * j] = jnp.where(first, low, pltpu.roll(high, width, 1)).astype(tiles.dtype)
        tiles[2 * j + 1] = jnp.where(first, pltpu.roll(low, width, 1), high).astype(tiles.dtype)
        if step == 0:
            wait_for_all()
        for copy in ready:
            copy.start()
        sends += ready
        if step == groups // 2:
            send_stats()
        if away:
            ready = [tile_to(2 * j), tile_to(2 * j + 1)]
        else:
            ready = [tile_to(2 * j + 1 - lax.rem(me, 2))]

    for copy in ready:
        copy.start()
    sends += ready

    lines = [stat[...]]
    for step in range(1, n):
        p = lax.rem(me + step, n)
        pltpu.make_async_remote_copy(
            src_ref=stat,
            dst_ref=stats.at[p],
            send_sem=s_send.at[p],
            recv_sem=s_recv.at[p],
            device_id={"corpus": p},
            device_id_type=MESH,
        ).wait_recv()
        lines.append(stats[p])
    top = functools.reduce(jnp.maximum, lines)
    line = top + jnp.log(sum(jnp.exp(item - top) for item in lines))
    column = jnp.sum(jnp.where(square, line, 0.0), axis=1, keepdims=True)
    total = tiles[me].astype(jnp.float32)
    for step in range(1, n):
        p = lax.rem(me + step, n)
        pltpu.make_async_remote_copy(
            src_ref=tiles.at[p],
            dst_ref=got.at[p],
            send_sem=t_send.at[p],
            recv_sem=t_recv.at[p],
            device_id={"corpus": p},
            device_id_type=MESH,
        ).wait_recv()
        total += got[p].astype(jnp.float32)
    result = total - jnp.where(first, column[:half], column[half:])
    out_ref[pl.ds(0, half), :] = result[:, :width]
    out_ref[pl.ds(half, half), :] = pltpu.roll(result, width, 1)[:, :width]

    for copy in swaps + sends:
        copy.wait_send()


def fused_body(n, queries, corpus, candidates):
    height, depth = queries.shape
    rows, feats = corpus.shape
    count = candidates.shape[1]
    parts = rows // LANES
    width = count // n
    dma = pltpu.SemaphoreType.DMA
    return pl.pallas_call(
        functools.partial(kernel, n),
        out_shape=jax.ShapeDtypeStruct((height, width), jnp.float32),
        in_specs=[pl.BlockSpec(memory_space=pltpu.HBM)] * 3,
        out_specs=pl.BlockSpec(memory_space=pltpu.VMEM),
        scratch_shapes=[
            pltpu.VMEM((height, depth), queries.dtype),
            pltpu.VMEM((rows, feats), corpus.dtype),
            pltpu.VMEM((rows, feats), corpus.dtype),
            pltpu.VMEM((height, count), jnp.int32),
            pltpu.VMEM((height, rows), jnp.float32),
            pltpu.VMEM((n, height // 2, LANES), jnp.bfloat16),
            pltpu.VMEM((n, height // 2, LANES), jnp.bfloat16),
            pltpu.VMEM((1, LANES), jnp.float32),
            pltpu.VMEM((n, 1, LANES), jnp.float32),
            pltpu.SemaphoreType.REGULAR((2,)),
            dma((2 + parts,)),
            dma((parts,)),
            dma((parts,)),
            dma((n,)),
            dma((n,)),
            dma((n,)),
            dma((n,)),
        ],
        compiler_params=pltpu.CompilerParams(
            collective_id=0, has_side_effects=True, vmem_limit_bytes=ROOM
        ),
    )(queries, corpus, candidates)


def body(n, cores, queries, corpus, candidates):
    dense = (
        cores == 2
        and candidates.shape[1] == n * LANES // 2
        and n >= 16
        and n & (n - 1) == 0
        and queries.shape[0] <= LANES
        and queries.shape[0] % 32 == 0
        and corpus.shape[0] % LANES == 0
        and corpus.shape[1] % LANES == 0
    )
    if dense:
        return fused_body(n, queries, corpus, candidates)
    return plain_body(queries, corpus, candidates)


def solution(mesh):
    placed = (P("dim", None), P("corpus", "dim"), P("dim", None))
    sized = functools.partial(body, mesh.shape["corpus"], mesh.shape["dim"])
    return jax.shard_map(
        sized, mesh=mesh, in_specs=placed, out_specs=P("dim", "corpus"), check_vma=False
    )
```

```python
import functools
import jax
import jax.numpy as jnp
from jax import lax
from jax.experimental import pallas as pl
from jax.experimental.pallas import tpu as pltpu
from jax.sharding import PartitionSpec as P

LANES = 128
ROOM = 55169 << 10
MESH = pl.DeviceIdType.MESH


def merged(value, axis, join):
    pieces = jax.tree.map(lambda part: lax.all_gather(part, axis), value)
    head = jax.tree.map(lambda part: part[0], pieces)
    tail = jax.tree.map(lambda part: part[1:], pieces)
    so_far, _ = lax.scan(lambda so_far, section: (join(so_far, section), None), head, tail)
    return so_far


def combine_pair(first, second):
    peak = jnp.maximum(first[0], second[0])
    mass = first[1] * jnp.exp(first[0] - peak) + second[1] * jnp.exp(second[0] - peak)
    return (peak, mass)


def local_pair(scores):
    peak = jnp.max(scores, axis=1)
    mass = jnp.sum(jnp.exp(scores - peak[:, None]), axis=1)
    return (peak, mass)


def pick_owned(scores, indices, offset):
    height = scores.shape[0]
    count = scores.shape[1]
    width = indices.shape[1]
    local = indices - offset
    inside = (local >= 0) & (local < count)
    upper = scores.astype(jnp.bfloat16)
    remain = scores - upper.astype(jnp.float32)
    middle = remain.astype(jnp.bfloat16)
    lower = (remain - middle.astype(jnp.float32)).astype(jnp.bfloat16)
    pieces = jnp.stack([upper, middle, lower], axis=1)
    group = 8

    def select_block(packed):
        block_pieces, block_local = packed
        positions = lax.broadcasted_iota(jnp.int32, (1, 1, count), 2)
        onehot = (block_local[:, :, None] == positions).astype(jnp.bfloat16)
        return jnp.einsum("qkr,qcr->qck", onehot, block_pieces, preferred_element_type=jnp.float32)

    selected = lax.map(
        select_block,
        (
            pieces.reshape(height // group, group, 3, count),
            local.reshape(height // group, group, width),
        ),
    )
    selected = selected.reshape(height, 3, width)
    values = selected[:, 2, :] + selected[:, 1, :] + selected[:, 0, :]
    return jnp.where(inside, values, jnp.float32(0.0))


def plain_body(queries, corpus, candidates):
    rows = corpus.shape[0]
    scores = lax.dot_general(
        queries,
        lax.all_gather(corpus, "dim", axis=1, tiled=True),
        (((1,), (1,)), ((), ())),
        preferred_element_type=jnp.float32,
    )
    peak, mass = merged(local_pair(scores), "corpus", combine_pair)
    own_lse = peak + jnp.log(mass)
    offset = lax.axis_index("corpus") * rows
    picked = pick_owned(scores, candidates, offset)
    logits = lax.psum_scatter(picked, "corpus", scatter_dimension=1, tiled=True)
    return logits - own_lse[:, None]


def times(left, right):
    return lax.dot_general(
        left, right, (((1,), (1,)), ((), ())), preferred_element_type=jnp.float32
    )


def kernel(
    n, q_hbm, c_hbm, k_hbm, out_ref,
    q, own, other, cand, scores, tiles, got, stat, stats,
    wave, load_sem, x_send, x_recv, t_send, t_recv, s_send, s_recv,
):
    me = lax.axis_index("corpus")
    side = lax.axis_index("dim")
    height = q.shape[0]
    rows, feats = own.shape
    width = cand.shape[1] // n
    parts = rows // LANES
    groups = cand.shape[1] // LANES
    half = height // 2

    def flipped(value, mask):
        for i in range(mask.bit_length()):
            bit = 1 << i
            if mask & bit:
                value = value + bit - 2 * bit * lax.rem(value // bit, 2)
        return value

    barrier = pltpu.get_barrier_semaphore()
    partner_in, all_in = wave.at[0], wave.at[1]

    def tell_partner(semaphore):
        pl.semaphore_signal(
            semaphore, inc=1, device_id={"dim": 1 - side}, device_id_type=MESH
        )

    @pl.when(side == 0)
    def _():
        tell_partner(barrier)

    def block(b):
        return pl.ds(b * LANES, LANES)

    load_q = pltpu.make_async_copy(q_hbm, q, load_sem.at[0])
    load_k = pltpu.make_async_copy(k_hbm, cand, load_sem.at[1])
    load_c = [
        pltpu.make_async_copy(c_hbm.at[block(b)], own.at[block(b)], load_sem.at[2 + b])
        for b in range(parts)
    ]
    for load in load_c:
        load.start()
    load_q.start()
    load_k.start()
    swaps = [
        pltpu.make_async_remote_copy(
            src_ref=own.at[block(b)],
            dst_ref=other.at[block(b)],
            send_sem=x_send.at[b],
            recv_sem=x_recv.at[b],
            device_id={"dim": 1 - side},
            device_id_type=MESH,
        )
        for b in range(parts)
    ]

    @pl.when(side == 1)
    def _():
        pl.semaphore_wait(barrier, 1)
        tell_partner(partner_in)

    @pl.when(side == 0)
    def _():
        pl.semaphore_wait(partner_in, 1)
        for step in range(1, n):
            pl.semaphore_signal(
                barrier, inc=1, device_id={"corpus": lax.rem(me + step, n)}, device_id_type=MESH
            )

    for b in range(parts):
        load_c[b].wait()
        swaps[b].start()
    load_q.wait()
    q_own = q[:, pl.ds(pl.multiple_of(side * feats, LANES), feats)]
    q_other = q[:, pl.ds(pl.multiple_of((1 - side) * feats, LANES), feats)]
    for b in range(parts):
        scores[:, block(b)] = times(q_own, own[block(b), :])
    load_k.wait()
    for b in range(parts):
        swaps[b].wait_recv()
        scores[:, block(b)] += times(q_other, other[block(b), :])

    def wait_for_all():
        @pl.when(side == 0)
        def _():
            pl.semaphore_wait(barrier, n - 1)
            tell_partner(all_in)

        @pl.when(side == 1)
        def _():
            pl.semaphore_wait(all_in, 1)

    def tile_to(p):
        return pltpu.make_async_remote_copy(
            src_ref=tiles.at[p],
            dst_ref=got.at[me],
            send_sem=t_send.at[p],
            recv_sem=t_recv.at[me],
            device_id={"corpus": p},
            device_id_type=MESH,
        )

    first = lax.broadcasted_iota(jnp.int32, (half, LANES), 1) < width
    square = lax.broadcasted_iota(jnp.int32, (height, LANES), 0) == lax.broadcasted_iota(
        jnp.int32, (height, LANES), 1
    )
    sends = []
    line_sends = []

    def make_stats():
        peak = jnp.max(scores[...], axis=1, keepdims=True)
        mass = jnp.sum(jnp.exp(scores[...] - peak), axis=1, keepdims=True)
        lse = peak + jnp.log(mass)
        stat[...] = jnp.sum(jnp.where(square, lse, 0.0), axis=0, keepdims=True)
        for step in range(1, n):
            p = lax.rem(me + step, n)
            copy = pltpu.make_async_remote_copy(
                src_ref=stat,
                dst_ref=stats.at[me],
                send_sem=s_send.at[p],
                recv_sem=s_recv.at[me],
                device_id={"corpus": p},
                device_id_type=MESH,
            )
            line_sends.append(copy)

    for step in range(groups):
        away = groups - 1 - step
        j = flipped(me // 2, away)
        local = cand[:, pl.ds(pl.multiple_of(j * LANES, LANES), LANES)] - me * rows
        lane = local & (LANES - 1)
        part = lax.shift_right_arithmetic(local, LANES.bit_length() - 1)
        picked = jnp.zeros((height, LANES), jnp.float32)
        for b in range(parts):
            found = jnp.take_along_axis(
                scores[:, block(b)], lane, axis=1, mode="promise_in_bounds"
            )
            picked = jnp.where(part == b, found, picked)
        low, high = picked[:half], picked[half:]
        tiles[2 * j] = jnp.where(first, low, pltpu.roll(high, width, 1)).astype(tiles.dtype)
        tiles[2 * j + 1] = jnp.where(first, pltpu.roll(low, width, 1), high).astype(tiles.dtype)
        if away:
            sends += [tile_to(2 * j), tile_to(2 * j + 1)]
        else:
            sends += [tile_to(2 * j + 1 - lax.rem(me, 2))]

    make_stats()
    wait_for_all()
    sends = sends[: n // 2] + line_sends + sends[n // 2 :]
    for copy in sends:
        copy.start()

    lines = [stat[...]]
    for step in range(1, n):
        p = lax.rem(me + step, n)
        pltpu.make_async_remote_copy(
            src_ref=stat,
            dst_ref=stats.at[p],
            send_sem=s_send.at[p],
            recv_sem=s_recv.at[p],
            device_id={"corpus": p},
            device_id_type=MESH,
        ).wait_recv()
        lines.append(stats[p])
    top = functools.reduce(jnp.maximum, lines)
    line = top + jnp.log(sum(jnp.exp(item - top) for item in lines))
    column = jnp.sum(jnp.where(square, line, 0.0), axis=1, keepdims=True)
    total = tiles[me].astype(jnp.float32)
    for step in range(1, n):
        p = lax.rem(me + step, n)
        pltpu.make_async_remote_copy(
            src_ref=tiles.at[p],
            dst_ref=got.at[p],
            send_sem=t_send.at[p],
            recv_sem=t_recv.at[p],
            device_id={"corpus": p},
            device_id_type=MESH,
        ).wait_recv()
        total += got[p].astype(jnp.float32)
    result = total - jnp.where(first, column[:half], column[half:])
    out_ref[pl.ds(0, half), :] = result[:, :width]
    out_ref[pl.ds(half, half), :] = pltpu.roll(result, width, 1)[:, :width]

    for copy in swaps + sends:
        copy.wait_send()


def fused_body(n, queries, corpus, candidates):
    height, depth = queries.shape
    rows, feats = corpus.shape
    count = candidates.shape[1]
    parts = rows // LANES
    width = count // n
    dma = pltpu.SemaphoreType.DMA
    return pl.pallas_call(
        functools.partial(kernel, n),
        out_shape=jax.ShapeDtypeStruct((height, width), jnp.float32),
        in_specs=[pl.BlockSpec(memory_space=pltpu.HBM)] * 3,
        out_specs=pl.BlockSpec(memory_space=pltpu.VMEM),
        scratch_shapes=[
            pltpu.VMEM((height, depth), queries.dtype),
            pltpu.VMEM((rows, feats), corpus.dtype),
            pltpu.VMEM((rows, feats), corpus.dtype),
            pltpu.VMEM((height, count), jnp.int32),
            pltpu.VMEM((height, rows), jnp.float32),
            pltpu.VMEM((n, height // 2, LANES), jnp.bfloat16),
            pltpu.VMEM((n, height // 2, LANES), jnp.bfloat16),
            pltpu.VMEM((1, LANES), jnp.float32),
            pltpu.VMEM((n, 1, LANES), jnp.float32),
            pltpu.SemaphoreType.REGULAR((2,)),
            dma((2 + parts,)),
            dma((parts,)),
            dma((parts,)),
            dma((n,)),
            dma((n,)),
            dma((n,)),
            dma((n,)),
        ],
        compiler_params=pltpu.CompilerParams(
            collective_id=0, has_side_effects=True, vmem_limit_bytes=ROOM
        ),
    )(queries, corpus, candidates)


def body(n, cores, queries, corpus, candidates):
    dense = (
        cores == 2
        and candidates.shape[1] == n * LANES // 2
        and n >= 16
        and n & (n - 1) == 0
        and queries.shape[0] <= LANES
        and queries.shape[0] % 32 == 0
        and corpus.shape[0] % LANES == 0
        and corpus.shape[1] % LANES == 0
    )
    if dense:
        return fused_body(n, queries, corpus, candidates)
    return plain_body(queries, corpus, candidates)


def solution(mesh):
    placed = (P("dim", None), P("corpus", "dim"), P("dim", None))
    sized = functools.partial(body, mesh.shape["corpus"], mesh.shape["dim"])
    return jax.shard_map(
        sized, mesh=mesh, in_specs=placed, out_specs=P("dim", "corpus"), check_vma=False
    )
```
